32 devices in a mesh: groups: 2 (over y), row: 4 (over z), head: 4 (over x, core).
Axes of the slice: x: 2, y: 2, z: 4, core: 2. Of those that a mesh axis runs over, the one named last changes fastest.
Arguments:
- tokens: bfloat16 [32, 2048], P('groups'), parts along dimension 0, may hold values from -6 to 6
- query_weight: bfloat16 [2048, 3072], P('row', 'head'), may hold values from -0.125 to 0.125
- latent_weight: bfloat16 [512, 4096], P('row', 'head'), may hold values from -0.25 to 0.25
- output_weight: bfloat16 [2048, 2048], P('row', 'head'), may hold values from -0.5 to 0.5
- cache_latent: bfloat16 [32, 2048, 512], P(('groups', 'row'), 'head'), parts along dimension 0, may hold values from -32 to 32
- cache_rope: bfloat16 [32, 64, 2048], P(('groups', 'row'), None, 'head'), parts along dimension 0, may hold values from -1800 to 1800
- lengths: int32 [32], P('groups'), parts along dimension 0, may hold values from 1 to 2048
- slot_seq: int32 [32], P('groups'), parts along dimension 0, may hold values from 0 to 15, each once
Outputs:
- attn_out: bfloat16 [32, 2048], P(('groups', 'row'), 'head'), parts along dimension 0
The draws below stay inside these ranges and needn't reach their ends.
There are 2 independent parts, one for each index of `groups`. The reference program is written for one: setup_inputs(seed, part) draws one part's arguments, and reference() takes and returns one part's arrays. A program takes and returns all parts, laid end to end along the dimension named above; an argument that names none is the same for every part. Nothing has to cross between parts.
Inputs may be any that keep to these rules, and one draw needn't show every extreme that they name: Cache row i belongs to sequence slot_seq[i], and output row i is that sequence's. Positions at or past lengths[s] of a sequence hold stale entries that are not read; its new token stands at position lengths[s] - 1.
All inputs are finite; a program needn't handle non-finite values.
Results may differ from the reference program's by a relative error of at most 0.039.
Values may be sent and summed in bfloat16 or wider, within the bound.
A program may use at most 64 MiB of HBM per device.

```python
import jax
import jax.numpy as jnp
from jax import lax

D = 2048
H = 16
NOPE = 128
ROPE = 64
V = 128
LAT = 512
B = 16
SMAX = 2048


def draw_cache_latent(key, part):
    values = jnp.clip(jax.random.normal(jax.random.fold_in(key, 11), (B, SMAX, LAT), jnp.float32), -8.0, 8.0)
    return values.astype(jnp.bfloat16)


def draw_cache_rope(key, part):
    values = jnp.clip(jax.random.normal(jax.random.fold_in(key, 21), (B, ROPE, SMAX), jnp.float32), -6.0, 6.0)
    return values.astype(jnp.bfloat16)


def plant(entries, key, smallest, top_value):
    shape = entries.shape
    place = [jax.random.randint(jax.random.fold_in(key, axis), (), 0, shape[axis]) for axis in range(len(shape))]
    entries = entries.at[tuple(place)].set(smallest)
    longest = shape.index(max(shape))
    place[longest] = (place[longest] + 1) % shape[longest]
    return entries.at[tuple(place)].set(top_value)


def shard_levels(rng, dims, pieces, smallest, high):
    factor_of = 1.0
    for dim, blocks in pieces:
        heights = jax.random.uniform(jax.random.fold_in(jax.random.fold_in(rng, 6), dim), (blocks,), jnp.float32, smallest / len(pieces), high / len(pieces))
        factor_of = factor_of * jnp.repeat(jnp.exp(heights), dims[dim] // blocks).reshape((-1,) + (1,) * (len(dims) - 1 - dim))
    return factor_of


def gaussian(own_key, shape, scale, limit, shards=(), kind=jnp.bfloat16):
    level = shard_levels(own_key, shape, shards, -0.22, 0.18) if shards else 1.0
    values = jax.random.normal(own_key, shape, jnp.float32) * scale * level
    return jnp.minimum(jnp.maximum(values, -limit), limit).astype(kind)


def setup_inputs(seed: int = 0, part: int = 0) -> dict:
    keys = jax.random.split(jax.random.key(seed), 9)
    part_splits = jax.random.split(jax.random.fold_in(keys[8], part), 9)
    tokens = gaussian(part_splits[0], (B, D), 1.0, 6.0)
    query_weight = gaussian(keys[1], (D, H * (NOPE + ROPE)), D ** -0.5, 0.125, ((0, 4), (1, 4)))
    latent_weight = gaussian(keys[2], (LAT, H * (NOPE + V)), LAT ** -0.5, 0.25, ((0, 4), (1, 4)))
    output_weight = gaussian(keys[3], (D, H * V), V ** -0.5, 0.5, ((0, 4), (1, 4)))
    cache_latent = draw_cache_latent(jax.random.fold_in(jax.random.fold_in(keys[8], part), 71), part)
    cache_rope = draw_cache_rope(jax.random.fold_in(jax.random.fold_in(keys[8], part), 71), part)
    lengths = plant(jax.random.randint(part_splits[6], (B,), 1, SMAX + 1), jax.random.fold_in(part_splits[6], 1), 1, SMAX).astype(jnp.int32)
    slot_seq = jax.random.permutation(part_splits[7], B).astype(jnp.int32)
    return dict(tokens=tokens, query_weight=query_weight, latent_weight=latent_weight, output_weight=output_weight, cache_latent=cache_latent, cache_rope=cache_rope, lengths=lengths, slot_seq=slot_seq)


neg_big = -1e+30

def absorb(query_weight, output_weight, kv_heads):
    width = query_weight.shape[0]
    head_total = kv_heads.shape[1]
    query_heads = query_weight.reshape(width, head_total, NOPE + ROPE)
    out_heads = output_weight.reshape(width, head_total, V)
    nope_part = jnp.einsum('dhn,lhn->dhl', query_heads[:, :, :NOPE].astype(jnp.float32), kv_heads[:, :, :NOPE].astype(jnp.float32)).astype(jnp.bfloat16)
    query_abs = jnp.concatenate([nope_part, query_heads[:, :, NOPE:]], axis=2).reshape(width, -1)
    out_abs = jnp.einsum('dhv,lhv->dhl', out_heads.astype(jnp.float32), kv_heads[:, :, NOPE:].astype(jnp.float32)).astype(jnp.bfloat16)
    return (query_abs, out_abs.reshape(width, -1))

def rotate(queries, seq_len):
    half_width = ROPE // 2
    inverse_freq = jnp.power(10000.0, -2.0 * jnp.arange(half_width, dtype=jnp.float32) / ROPE)
    angles = (seq_len - 1).astype(jnp.float32)[:, None] * inverse_freq[None, :]
    cosine = jnp.cos(angles)[:, None, :]
    sine = jnp.sin(angles)[:, None, :]
    first_half = queries[:, :, LAT:LAT + half_width]
    second_half = queries[:, :, LAT + half_width:]
    rotated = jnp.concatenate([first_half * cosine - second_half * sine, first_half * sine + second_half * cosine], axis=2)
    return jnp.concatenate([queries[:, :, :LAT], rotated], axis=2)

def reference(tokens, query_weight, latent_weight, output_weight, cache_latent, cache_rope, lengths, slot_seq):
    kv_heads = latent_weight.reshape(LAT, H, NOPE + V)
    query_abs, out_abs = absorb(query_weight, output_weight, kv_heads)
    chosen = tokens[slot_seq]
    seq_len = lengths[slot_seq].astype(jnp.int32)
    queries = jnp.dot(chosen, query_abs, preferred_element_type=jnp.float32).reshape(B, H, LAT + ROPE)
    queries = rotate(queries, seq_len).astype(jnp.bfloat16)
    positions = jnp.arange(SMAX, dtype=jnp.int32)
    score_scale = 1.0 / jnp.sqrt(jnp.float32(NOPE + ROPE))

    def attend(inputs_one):
        query_one, latent_one, rope_one, length_one = inputs_one
        scores = jnp.dot(query_one[:, :LAT], latent_one.T, preferred_element_type=jnp.float32)
        scores = (scores + jnp.dot(query_one[:, LAT:], rope_one, preferred_element_type=jnp.float32)) * score_scale
        in_range = positions[None, :] < length_one
        masked = jnp.where(in_range, scores, neg_big)
        peak_max = lax.optimization_barrier(jnp.max(masked, axis=1, keepdims=True))
        weights = jnp.where(in_range, jnp.exp(masked - peak_max), 0.0)
        total = lax.optimization_barrier(jnp.sum(weights, axis=1))
        summed = jnp.dot(weights.astype(jnp.bfloat16), latent_one, preferred_element_type=jnp.float32)
        return (summed / total[:, None]).astype(jnp.bfloat16)
    latent_out = lax.map(attend, (queries, cache_latent, cache_rope, seq_len))
    attn_out = jnp.einsum('bhl,dhl->bd', latent_out.astype(jnp.float32), out_abs.reshape(D, H, LAT).astype(jnp.float32))
    return attn_out.astype(jnp.bfloat16)
```

```python
import functools

import jax
import jax.numpy as jnp
import numpy as np
from jax import lax
from jax.experimental import pallas as pl
from jax.experimental.pallas import tpu as pltpu
from jax.sharding import PartitionSpec as P

D = 2048
H = 16
NOPE = 128
ROPE = 64
V = 128
LAT = 512
BLOCK = 256


neg_big = -1e30


def combined_all(part, axis, combine):
    gathered = jax.tree.map(lambda a: lax.all_gather(a, axis), part)

    def take(source):
        return jax.tree.map(lambda a: lax.dynamic_index_in_dim(a, source, 0, False), gathered)

    return lax.fori_loop(
        1, lax.axis_size(axis), lambda source, state: combine(state, take(source)), take(0)
    )


def absorb(query_weight, output_weight, kv_heads):
    width = query_weight.shape[0]
    head_total = kv_heads.shape[1]
    query_heads = query_weight.reshape(width, head_total, NOPE + ROPE)
    out_heads = output_weight.reshape(width, head_total, V)
    nope_part = jnp.einsum(
        "dhn,lhn->dhl",
        query_heads[:, :, :NOPE],
        kv_heads[:, :, :NOPE],
        preferred_element_type=jnp.float32,
    ).astype(jnp.bfloat16)
    query_abs = jnp.concatenate([nope_part, query_heads[:, :, NOPE:]], axis=2).reshape(width, -1)
    out_abs = jnp.einsum(
        "dhv,lhv->dhl", out_heads, kv_heads[:, :, NOPE:], preferred_element_type=jnp.float32
    ).astype(jnp.bfloat16)
    return (query_abs, out_abs.reshape(width, -1))


def rotate(queries, seq_len):
    half_width = ROPE // 2
    inverse_freq = jnp.power(10000.0, -2.0 * jnp.arange(half_width, dtype=jnp.float32) / ROPE)
    angles = (seq_len - 1).astype(jnp.float32)[:, None] * inverse_freq[None, :]
    cosine = jnp.cos(angles)[:, None, :]
    sine = jnp.sin(angles)[:, None, :]
    first_half = queries[:, :, LAT : LAT + half_width]
    second_half = queries[:, :, LAT + half_width :]
    rotated = jnp.concatenate(
        [first_half * cosine - second_half * sine, first_half * sine + second_half * cosine], axis=2
    )
    return jnp.concatenate([queries[:, :, :LAT], rotated], axis=2)


def combine(earlier, later):
    earlier_max, earlier_sum, earlier_acc = earlier
    later_max, later_sum, later_acc = later
    peak_max = jnp.maximum(earlier_max, later_max)
    earlier_scale = jnp.exp(earlier_max - peak_max)
    later_scale = jnp.exp(later_max - peak_max)
    summed = earlier_sum * earlier_scale + later_sum * later_scale
    weighted = earlier_acc * earlier_scale[..., None] + later_acc * later_scale[..., None]
    return (peak_max, summed, weighted)


def local(
    tokens, query_weight, latent_weight, output_weight, cache_latent, cache_rope, lengths, slot_seq
):
    heads_dev = query_weight.shape[1] // (NOPE + ROPE)
    seq_dev = cache_latent.shape[0]
    seg_len = cache_latent.shape[1]
    latent_full = lax.all_gather(latent_weight, "row", axis=0, tiled=True)
    kv_heads = latent_full.reshape(LAT, heads_dev, NOPE + V)
    full_query, full_out = (
        lax.all_gather(query_weight, "row", axis=0, tiled=True),
        lax.all_gather(output_weight, "row", axis=0, tiled=True),
    )
    query_abs, out_abs = absorb(full_query, full_out, kv_heads)
    first_row = lax.axis_index("row") * seq_dev
    seq_ids = lax.dynamic_slice_in_dim(slot_seq, first_row, seq_dev)
    chosen = tokens[seq_ids]
    seq_len = lengths[seq_ids]
    queries = jnp.dot(chosen, query_abs, preferred_element_type=jnp.float32).reshape(
        seq_dev, heads_dev, LAT + ROPE
    )
    queries = (
        rotate(queries, seq_len).astype(jnp.bfloat16).reshape(seq_dev, heads_dev * (LAT + ROPE))
    )
    queries = lax.all_gather(queries, "head", axis=1, tiled=True).reshape(seq_dev, H, LAT + ROPE)
    query_latent = queries[:, :, :LAT]
    query_rope = queries[:, :, LAT:]
    score_scale = 1.0 / jnp.sqrt(jnp.float32(NOPE + ROPE))
    offset = lax.axis_index("head") * seg_len
    local_len = jnp.clip(seq_len - offset, 0, seg_len)
    live_blocks = (jnp.max(local_len) + BLOCK - 1) // BLOCK

    def advance(block_idx, running):
        run_max, run_sum, run_acc = running
        begin_at = block_idx * BLOCK
        latent_blk = lax.dynamic_slice_in_dim(cache_latent, begin_at, BLOCK, 1)
        rope_blk = lax.dynamic_slice_in_dim(cache_rope, begin_at, BLOCK, 2)
        scores = jnp.einsum(
            "bhl,btl->bht", query_latent, latent_blk, preferred_element_type=jnp.float32
        )
        scores = (
            scores
            + jnp.einsum("bhr,brt->bht", query_rope, rope_blk, preferred_element_type=jnp.float32)
        ) * score_scale
        in_range = (begin_at + jnp.arange(BLOCK, dtype=jnp.int32))[None, None, :] < local_len[
            :, None, None
        ]
        masked = jnp.where(in_range, scores, neg_big)
        new_max = jnp.maximum(run_max, jnp.max(masked, axis=2))
        weights = jnp.where(in_range, jnp.exp(masked - new_max[..., None]), 0.0)
        factor = jnp.exp(run_max - new_max)
        run_sum = run_sum * factor + jnp.sum(weights, axis=2)
        run_acc = run_acc * factor[..., None] + jnp.einsum(
            "bht,btl->bhl",
            weights.astype(jnp.bfloat16),
            latent_blk,
            preferred_element_type=jnp.float32,
        )
        return (new_max, run_sum, run_acc)

    initial = (
        jnp.full((seq_dev, H), neg_big, jnp.float32),
        jnp.zeros((seq_dev, H), jnp.float32),
        jnp.zeros((seq_dev, H, LAT), jnp.float32),
    )
    partial_state = lax.fori_loop(0, live_blocks, advance, initial)
    merged_max, merged_sum, merged_acc = combined_all(partial_state, "head", combine)
    latent_out = (merged_acc / merged_sum[..., None]).astype(jnp.bfloat16)
    own_heads = lax.dynamic_slice_in_dim(
        latent_out, lax.axis_index("head") * heads_dev, heads_dev, 1
    )
    out_term = jnp.einsum(
        "bhl,dhl->bd",
        own_heads,
        out_abs.reshape(D, heads_dev, LAT),
        preferred_element_type=jnp.float32,
    )
    return lax.psum_scatter(out_term, "head", scatter_dimension=1, tiled=True).astype(jnp.bfloat16)


F32 = jnp.float32
BF16 = jnp.bfloat16
MESH = pl.DeviceIdType.MESH


def dot_nn(a, b):
    return lax.dot_general(a, b, (((1,), (0,)), ((), ())), preferred_element_type=F32)


def dot_nt(a, b):
    return lax.dot_general(a, b, (((1,), (1,)), ((), ())), preferred_element_type=F32)


def iota(shape, axis):
    return lax.broadcasted_iota(jnp.int32, shape, axis)


def fused(
    nr, nh, sd, hd,
    freq_h, tok_h, wq_h, wl_h, wo_h, cl_h, cr_h, len_h, slot_h,
    out_ref,
    freq, tok, wq, wl, wo, cl, cr, lens, slot,
    a_send, a_recv, ar_send, ar_recv,
    b_send, b_recv, br_send, br_recv,
    st_send, st_recv, d_send, d_recv,
    e_send, e_recv, f_send, f_recv,
    load_sem,
    a_ss, a_rs, ar_ss, ar_rs, b_ss, b_rs, br_ss, br_rs,
    st_ss, st_rs, d_ss, d_rs, e_ss, e_rs, f_ss, f_rs,
):
    r = lax.axis_index("row")
    h = lax.axis_index("head")
    batch = nr * sd
    rows = sd * hd
    db = wq.shape[0]
    seg = cl.shape[1]
    lb = LAT // nr

    def load(k, src, dst):
        c = pltpu.make_async_copy(src, dst, load_sem.at[k])
        c.start()
        return c

    ld_slot = load(0, slot_h, slot)
    ld_len = load(1, len_h, lens)
    ld_tok = load(2, tok_h.at[:, pl.ds(pl.multiple_of(r * db, 128), db)], tok)
    ld_wq = load(3, wq_h, wq)
    ld_freq = load(4, freq_h, freq)
    ld_wl = load(5, wl_h, wl)
    ld_cl = load(6, cl_h, cl)
    ld_cr = load(7, cr_h, cr)
    ld_wo = load(8, wo_h, wo)

    order = [dr for dr in range(nr) if dr] + [0]
    pairs = [(dr, dh) for dr in order for dh in range(nh) if dr or dh]
    barrier = pltpu.get_barrier_semaphore()
    for dr, dh in pairs:
        pl.semaphore_signal(
            barrier, inc=1,
            device_id={"row": lax.rem(r + dr, nr), "head": lax.rem(h + dh, nh)},
            device_id_type=MESH,
        )
    pending = []

    def send(src, dst, ss, rs, dr, dh):
        c = pltpu.make_async_remote_copy(
            src_ref=src, dst_ref=dst, send_sem=ss, recv_sem=rs,
            device_id={"row": lax.rem(r + dr, nr), "head": lax.rem(h + dh, nh)},
            device_id_type=MESH,
        )
        c.start()
        pending.append(c)
        return c

    ld_slot.wait()
    ld_len.wait()
    ld_tok.wait()
    pick_row = iota((batch, batch), 0)
    picked = jnp.zeros((batch, batch), jnp.int32)
    for i in range(batch):
        picked = jnp.where(pick_row == i, slot[i], picked)
    pick = (iota((batch, batch), 1) == picked).astype(F32).astype(BF16)
    chosen = dot_nn(pick, tok[...]).astype(BF16)
    ld_wq.wait()
    part = dot_nn(chosen, wq[...])
    width = NOPE + ROPE
    nope = jnp.concatenate([part[:, width * j : width * j + NOPE] for j in range(hd)], axis=1)
    rope = jnp.concatenate([part[:, width * j + NOPE : width * (j + 1)] for j in range(hd)], axis=1)
    a_send[...] = nope.astype(BF16)
    for k in range(nr):
        ar_send[k] = rope[k * sd : (k + 1) * sd, :]
    pl.semaphore_wait(barrier, len(pairs))
    copies = []
    for dr in order[:-1]:
        copies.append(send(a_send, a_recv.at[dr - 1], a_ss.at[dr], a_rs.at[dr], dr, 0))
    for dr in order[:-1]:
        copies.append(
            send(ar_send.at[lax.rem(r + dr, nr)], ar_recv.at[dr - 1], ar_ss.at[dr], ar_rs.at[dr], dr, 0)
        )
    n_own = [lens[slot[r * sd + i]] for i in range(sd)]
    half = ROPE // 2
    ld_freq.wait()
    seq_of = lax.rem(iota((rows, half), 0), sd)
    pos = jnp.zeros((rows, half), jnp.int32)
    for i in range(sd):
        pos = jnp.where(seq_of == i, n_own[i] - 1, pos)
    angles = pos.astype(F32) * freq[...]
    cosine = jnp.cos(angles)
    sine = jnp.sin(angles)
    rope_own = ar_send[r]
    ld_wl.wait()
    for c in copies:
        c.wait_recv()
    for k in range(nr - 1):
        nope = nope + a_recv[k].astype(F32)
        rope_own = rope_own + ar_recv[k]

    turned = jnp.concatenate([rope_own[:, ROPE * j : ROPE * (j + 1)] for j in range(hd)], axis=0)
    first, second = turned[:, :half], turned[:, half:]
    turned = jnp.concatenate(
        [first * cosine - second * sine, first * sine + second * cosine, jnp.zeros((rows, 128 - ROPE), F32)],
        axis=1,
    ).astype(BF16)
    br_send[...] = turned
    br_recv[h] = turned
    nope = nope.astype(BF16)
    absorbed = [
        dot_nt(nope[:, NOPE * j : NOPE * (j + 1)], wl[:, (NOPE + V) * j : (NOPE + V) * j + NOPE])
        for j in range(hd)
    ]
    for k in range(nr):
        b_send[k] = jnp.concatenate([x[k * sd : (k + 1) * sd] for x in absorbed], axis=0).astype(BF16)
    copies = []
    for k, (dr, dh) in enumerate(pairs):
        copies.append(
            send(b_send.at[lax.rem(r + dr, nr)], b_recv.at[r, h], b_ss.at[k], b_rs.at[k], dr, dh)
        )
    for dh in range(1, nh):
        copies.append(send(br_send, br_recv.at[h], br_ss.at[dh], br_rs.at[dh], 0, dh))
    b_recv[r, h] = b_send[r]
    ld_cl.wait()
    ld_cr.wait()
    total_rows = nh * rows
    lane_pos = iota((total_rows, seg), 1) + h * seg
    row_seq = lax.rem(iota((total_rows, seg), 0), sd)
    limit = jnp.zeros((total_rows, seg), jnp.int32)
    for i in range(sd):
        limit = jnp.where(row_seq == i, n_own[i], limit)
    in_range = lane_pos < limit
    for c in copies:
        c.wait_recv()

    query = jnp.concatenate(
        [
            jnp.concatenate([b_recv[k, g] for g in range(nh)], axis=0)
            for k in range(nr)
        ],
        axis=1,
    )
    query_rope = jnp.concatenate([br_recv[g] for g in range(nh)], axis=0)[:, :ROPE]
    scores = jnp.zeros((total_rows, seg), F32)
    for i in range(sd):
        s_i = dot_nt(query, cl[i]) + dot_nn(query_rope, cr[i])
        scores = jnp.where(row_seq == i, s_i, scores)
    scores = jnp.where(in_range, scores * np.float32(1.0 / np.sqrt(NOPE + ROPE)), neg_big)
    peak = jnp.max(scores, axis=1, keepdims=True)
    weights = jnp.where(in_range, jnp.exp(scores - peak), 0.0)
    summed = jnp.sum(weights, axis=1, keepdims=True)
    diag = iota((total_rows, 128), 0) == iota((total_rows, 128), 1)
    peak_row = jnp.sum(jnp.where(diag, peak, 0.0), axis=0, keepdims=True)
    sum_row = jnp.sum(jnp.where(diag, summed, 0.0), axis=0, keepdims=True)
    stat = jnp.where(iota((8, 128), 0) == 0, peak_row, sum_row)
    st_send[...] = stat
    copies = [
        send(st_send, st_recv.at[dh - 1], st_ss.at[dh], st_rs.at[dh], 0, dh) for dh in range(1, nh)
    ]
    weights = weights.astype(BF16)
    acc = jnp.zeros((total_rows, LAT), F32)
    out_seq = lax.rem(iota((total_rows, LAT), 0), sd)
    for i in range(sd):
        acc = jnp.where(out_seq == i, dot_nn(weights, cl[i]), acc)
    for c in copies:
        c.wait_recv()
    peaks = [peak_row] + [st_recv[k, 0:1, :] for k in range(nh - 1)]
    sums = [sum_row] + [st_recv[k, 1:2, :] for k in range(nh - 1)]
    top = functools.reduce(jnp.maximum, peaks)
    total = functools.reduce(jnp.add, [s * jnp.exp(p - top) for p, s in zip(peaks, sums)])
    lane_ok = iota((1, 128), 1) < total_rows
    factor_row = jnp.where(lane_ok, jnp.exp(peak_row - top) / jnp.where(lane_ok, total, 1.0), 0.0)
    factor = jnp.sum(jnp.where(diag, factor_row, 0.0), axis=1, keepdims=True)
    acc = (acc * factor).astype(BF16)
    for g in range(nh):
        for k in range(nr):
            d_send[k, g] = acc[g * rows : (g + 1) * rows, k * lb : (k + 1) * lb]
    copies = []
    for k, (dr, dh) in enumerate(pairs):
        copies.append(
            send(
                d_send.at[lax.rem(r + dr, nr), lax.rem(h + dh, nh)],
                d_recv.at[r, h], d_ss.at[k], d_rs.at[k], dr, dh,
            )
        )
    d_recv[r, h] = d_send[r, h]
    for c in copies:
        c.wait_recv()

    latent = [
        functools.reduce(jnp.add, [d_recv[k, g].astype(F32) for g in range(nh)]) for k in range(nr)
    ]
    context = jnp.concatenate(
        [
            dot_nn(
                jnp.concatenate([x[sd * j : sd * (j + 1)] for x in latent], axis=0).astype(BF16),
                wl[:, (NOPE + V) * j + NOPE : (NOPE + V) * (j + 1)],
            )
            for j in range(hd)
        ],
        axis=1,
    )
    e_send[...] = context.astype(BF16)
    copies = [
        send(e_send, e_recv.at[dr - 1], e_ss.at[dr], e_rs.at[dr], dr, 0) for dr in order[:-1]
    ]
    ld_wo.wait()
    for c in copies:
        c.wait_recv()
    for k in range(nr - 1):
        context = context + e_recv[k].astype(F32)
    out_part = dot_nt(context.astype(BF16), wo[...])
    for k in range(nr):
        f_send[k] = out_part[k * sd : (k + 1) * sd, :]

    def final(k, slot_at):
        return pltpu.make_async_remote_copy(
            src_ref=f_send.at[k], dst_ref=f_recv.at[slot_at],
            send_sem=f_ss.at[k], recv_sem=f_rs.at[slot_at],
            device_id={"row": k, "head": r}, device_id_type=MESH,
        )

    for k in range(nr):
        mine = jnp.logical_and(r == k, h == r)

        @pl.when(jnp.logical_not(mine))
        def _():
            final(k, h).start()

        @pl.when(mine)
        def _():
            f_recv[h] = f_send[k]

    for c in pending:
        c.wait_send()
    for g in range(nh):

        @pl.when(jnp.logical_not(jnp.logical_and(h == r, h == g)))
        def _():
            final(0, g).wait_recv()

    out_ref[...] = functools.reduce(jnp.add, [f_recv[g] for g in range(nh)])
    for k in range(nr):

        @pl.when(jnp.logical_not(jnp.logical_and(r == k, h == r)))
        def _():
            final(k, h).wait_send()


def local_fused(
    nr, nh,
    tokens, query_weight, latent_weight, output_weight, cache_latent, cache_rope, lengths, slot_seq
):
    sd, seg, _ = cache_latent.shape
    hd = query_weight.shape[1] // (NOPE + ROPE)
    batch = nr * sd
    rows = sd * hd
    lb = LAT // nr
    db = query_weight.shape[0]
    half = ROPE // 2
    freq = np.power(10000.0, -2.0 * np.arange(half, dtype=np.float32) / ROPE).astype(np.float32)
    vm = pltpu.VMEM
    dma = pltpu.SemaphoreType.DMA
    pairs = nr * nh - 1
    scratch = [
        vm((1, half), F32),
        vm((batch, db), BF16),
        vm(query_weight.shape, BF16),
        vm(latent_weight.shape, BF16),
        vm(output_weight.shape, BF16),
        vm(cache_latent.shape, BF16),
        vm(cache_rope.shape, BF16),
        pltpu.SMEM(lengths.shape, jnp.int32),
        pltpu.SMEM(slot_seq.shape, jnp.int32),
        vm((batch, hd * NOPE), BF16),
        vm((nr - 1, batch, hd * NOPE), BF16),
        vm((nr, sd, hd * ROPE), F32),
        vm((nr - 1, sd, hd * ROPE), F32),
        vm((nr, rows, lb), BF16),
        vm((nr, nh, rows, lb), BF16),
        vm((rows, 128), BF16),
        vm((nh, rows, 128), BF16),
        vm((8, 128), F32),
        vm((nh - 1, 8, 128), F32),
        vm((nr, nh, rows, lb), BF16),
        vm((nr, nh, rows, lb), BF16),
        vm((batch, hd * V), BF16),
        vm((nr - 1, batch, hd * V), BF16),
        vm((nr, sd, db), F32),
        vm((nh, sd, db), F32),
        dma((9,)),
    ]
    for count in (nr, nr, pairs, nh, nh, pairs, nr, max(nr, nh)):
        scratch += [dma((count,)), dma((count,))]
    anywhere = pl.BlockSpec(memory_space=pl.ANY)
    summed = pl.pallas_call(
        functools.partial(fused, nr, nh, sd, hd),
        out_shape=jax.ShapeDtypeStruct((sd, db), F32),
        in_specs=[anywhere] * 9,
        out_specs=pl.BlockSpec(memory_space=pltpu.VMEM),
        scratch_shapes=scratch,
        compiler_params=pltpu.CompilerParams(collective_id=0, has_side_effects=True),
    )(
        jnp.asarray(freq)[None, :], tokens, query_weight, latent_weight, output_weight,
        cache_latent, cache_rope, lengths, slot_seq,
    )
    return summed.astype(BF16)


def solution(mesh):
    placed = (
        P("groups", None),
        P("row", "head"),
        P("row", "head"),
        P("row", "head"),
        P(("groups", "row"), "head", None),
        P(("groups", "row"), None, "head"),
        P("groups"),
        P("groups"),
    )
    nr, nh = mesh.shape["row"], mesh.shape["head"]
    square = nr == nh and nr > 1 and (LAT // nr) % 128 == 0

    def choose(*args):
        query_weight, cache_latent = args[1], args[4]
        rows = cache_latent.shape[0] * (query_weight.shape[1] // (NOPE + ROPE))
        if square and rows % 16 == 0 and rows * nh <= 128:
            return local_fused(nr, nh, *args)
        return local(*args)

    return jax.shard_map(
        choose, mesh=mesh, in_specs=placed, out_specs=P(("groups", "row"), "head"), check_vma=False
    )
```

```python
import functools

import jax
import jax.numpy as jnp
import numpy as np
from jax import lax
from jax.experimental import pallas as pl
from jax.experimental.pallas import tpu as pltpu
from jax.sharding import PartitionSpec as P

D = 2048
H = 16
NOPE = 128
ROPE = 64
V = 128
LAT = 512
BLOCK = 256


neg_big = -1e30


def combined_all(part, axis, combine):
    gathered = jax.tree.map(lambda a: lax.all_gather(a, axis), part)

    def take(source):
        return jax.tree.map(lambda a: lax.dynamic_index_in_dim(a, source, 0, False), gathered)

    return lax.fori_loop(
        1, lax.axis_size(axis), lambda source, state: combine(state, take(source)), take(0)
    )


def absorb(query_weight, output_weight, kv_heads):
    width = query_weight.shape[0]
    head_total = kv_heads.shape[1]
    query_heads = query_weight.reshape(width, head_total, NOPE + ROPE)
    out_heads = output_weight.reshape(width, head_total, V)
    nope_part = jnp.einsum(
        "dhn,lhn->dhl",
        query_heads[:, :, :NOPE],
        kv_heads[:, :, :NOPE],
        preferred_element_type=jnp.float32,
    ).astype(jnp.bfloat16)
    query_abs = jnp.concatenate([nope_part, query_heads[:, :, NOPE:]], axis=2).reshape(width, -1)
    out_abs = jnp.einsum(
        "dhv,lhv->dhl", out_heads, kv_heads[:, :, NOPE:], preferred_element_type=jnp.float32
    ).astype(jnp.bfloat16)
    return (query_abs, out_abs.reshape(width, -1))


def rotate(queries, seq_len):
    half_width = ROPE // 2
    inverse_freq = jnp.power(10000.0, -2.0 * jnp.arange(half_width, dtype=jnp.float32) / ROPE)
    angles = (seq_len - 1).astype(jnp.float32)[:, None] * inverse_freq[None, :]
    cosine = jnp.cos(angles)[:, None, :]
    sine = jnp.sin(angles)[:, None, :]
    first_half = queries[:, :, LAT : LAT + half_width]
    second_half = queries[:, :, LAT + half_width :]
    rotated = jnp.concatenate(
        [first_half * cosine - second_half * sine, first_half * sine + second_half * cosine], axis=2
    )
    return jnp.concatenate([queries[:, :, :LAT], rotated], axis=2)


def combine(earlier, later):
    earlier_max, earlier_sum, earlier_acc = earlier
    later_max, later_sum, later_acc = later
    peak_max = jnp.maximum(earlier_max, later_max)
    earlier_scale = jnp.exp(earlier_max - peak_max)
    later_scale = jnp.exp(later_max - peak_max)
    summed = earlier_sum * earlier_scale + later_sum * later_scale
    weighted = earlier_acc * earlier_scale[..., None] + later_acc * later_scale[..., None]
    return (peak_max, summed, weighted)


def local(
    tokens, query_weight, latent_weight, output_weight, cache_latent, cache_rope, lengths, slot_seq
):
    heads_dev = query_weight.shape[1] // (NOPE + ROPE)
    seq_dev = cache_latent.shape[0]
    seg_len = cache_latent.shape[1]
    latent_full = lax.all_gather(latent_weight, "row", axis=0, tiled=True)
    kv_heads = latent_full.reshape(LAT, heads_dev, NOPE + V)
    full_query, full_out = (
        lax.all_gather(query_weight, "row", axis=0, tiled=True),
        lax.all_gather(output_weight, "row", axis=0, tiled=True),
    )
    query_abs, out_abs = absorb(full_query, full_out, kv_heads)
    first_row = lax.axis_index("row") * seq_dev
    seq_ids = lax.dynamic_slice_in_dim(slot_seq, first_row, seq_dev)
    chosen = tokens[seq_ids]
    seq_len = lengths[seq_ids]
    queries = jnp.dot(chosen, query_abs, preferred_element_type=jnp.float32).reshape(
        seq_dev, heads_dev, LAT + ROPE
    )
    queries = (
        rotate(queries, seq_len).astype(jnp.bfloat16).reshape(seq_dev, heads_dev * (LAT + ROPE))
    )
    queries = lax.all_gather(queries, "head", axis=1, tiled=True).reshape(seq_dev, H, LAT + ROPE)
    query_latent = queries[:, :, :LAT]
    query_rope = queries[:, :, LAT:]
    score_scale = 1.0 / jnp.sqrt(jnp.float32(NOPE + ROPE))
    offset = lax.axis_index("head") * seg_len
    local_len = jnp.clip(seq_len - offset, 0, seg_len)
    live_blocks = (jnp.max(local_len) + BLOCK - 1) // BLOCK

    def advance(block_idx, running):
        run_max, run_sum, run_acc = running
        begin_at = block_idx * BLOCK
        latent_blk = lax.dynamic_slice_in_dim(cache_latent, begin_at, BLOCK, 1)
        rope_blk = lax.dynamic_slice_in_dim(cache_rope, begin_at, BLOCK, 2)
        scores = jnp.einsum(
            "bhl,btl->bht", query_latent, latent_blk, preferred_element_type=jnp.float32
        )
        scores = (
            scores
            + jnp.einsum("bhr,brt->bht", query_rope, rope_blk, preferred_element_type=jnp.float32)
        ) * score_scale
        in_range = (begin_at + jnp.arange(BLOCK, dtype=jnp.int32))[None, None, :] < local_len[
            :, None, None
        ]
        masked = jnp.where(in_range, scores, neg_big)
        new_max = jnp.maximum(run_max, jnp.max(masked, axis=2))
        weights = jnp.where(in_range, jnp.exp(masked - new_max[..., None]), 0.0)
        factor = jnp.exp(run_max - new_max)
        run_sum = run_sum * factor + jnp.sum(weights, axis=2)
        run_acc = run_acc * factor[..., None] + jnp.einsum(
            "bht,btl->bhl",
            weights.astype(jnp.bfloat16),
            latent_blk,
            preferred_element_type=jnp.float32,
        )
        return (new_max, run_sum, run_acc)

    initial = (
        jnp.full((seq_dev, H), neg_big, jnp.float32),
        jnp.zeros((seq_dev, H), jnp.float32),
        jnp.zeros((seq_dev, H, LAT), jnp.float32),
    )
    partial_state = lax.fori_loop(0, live_blocks, advance, initial)
    merged_max, merged_sum, merged_acc = combined_all(partial_state, "head", combine)
    latent_out = (merged_acc / merged_sum[..., None]).astype(jnp.bfloat16)
    own_heads = lax.dynamic_slice_in_dim(
        latent_out, lax.axis_index("head") * heads_dev, heads_dev, 1
    )
    out_term = jnp.einsum(
        "bhl,dhl->bd",
        own_heads,
        out_abs.reshape(D, heads_dev, LAT),
        preferred_element_type=jnp.float32,
    )
    return lax.psum_scatter(out_term, "head", scatter_dimension=1, tiled=True).astype(jnp.bfloat16)


F32 = jnp.float32
BF16 = jnp.bfloat16
MESH = pl.DeviceIdType.MESH


def dot_nn(a, b):
    return lax.dot_general(a, b, (((1,), (0,)), ((), ())), preferred_element_type=F32)


def dot_nt(a, b):
    return lax.dot_general(a, b, (((1,), (1,)), ((), ())), preferred_element_type=F32)


def iota(shape, axis):
    return lax.broadcasted_iota(jnp.int32, shape, axis)


def fused(
    nr, nh, sd, hd,
    freq_h, tok_h, wq_h, wl_h, wo_h, cl_h, cr_h, len_h, slot_h,
    out_ref,
    freq, tok, wq, wl, wo, cl, cr, lens, slot,
    a_send, a_recv, ar_send, ar_recv,
    b_send, b_recv, br_send, br_recv,
    st_send, st_recv, d_send, d_recv,
    e_send, e_recv, f_send, f_recv,
    load_sem,
    send_sem, recv_sem,
):
    r = lax.axis_index("row")
    h = lax.axis_index("head")
    batch = nr * sd
    rows = sd * hd
    db = wq.shape[0]
    seg = cl.shape[1]
    lb = LAT // nr

    def load(k, src, dst):
        c = pltpu.make_async_copy(src, dst, load_sem.at[k])
        c.start()
        return c

    ld_slot = load(0, slot_h, slot)
    ld_len = load(1, len_h, lens)
    ld_tok = load(2, tok_h.at[:, pl.ds(pl.multiple_of(r * db, 128), db)], tok)
    ld_wq = load(3, wq_h, wq)
    ld_freq = load(4, freq_h, freq)
    ld_wl = load(5, wl_h, wl)
    ld_cl = load(6, cl_h, cl)
    ld_cr = load(7, cr_h, cr)
    ld_wo = load(8, wo_h, wo)

    order = [dr for dr in range(nr) if dr] + [0]
    pairs = [(dr, dh) for dr in order for dh in range(nh) if dr or dh]
    barrier = pltpu.get_barrier_semaphore()
    for dr, dh in pairs:
        pl.semaphore_signal(
            barrier, inc=1,
            device_id={"row": lax.rem(r + dr, nr), "head": lax.rem(h + dh, nh)},
            device_id_type=MESH,
        )

    def send(phase, src, dst, dr, dh):
        pltpu.make_async_remote_copy(
            src_ref=src, dst_ref=dst, send_sem=send_sem.at[phase], recv_sem=recv_sem.at[phase],
            device_id={"row": lax.rem(r + dr, nr), "head": lax.rem(h + dh, nh)},
            device_id_type=MESH,
        ).start()

    def span(phase, ref, count):
        return pltpu.make_async_remote_copy(
            src_ref=ref.at[pl.ds(0, count)], dst_ref=ref.at[pl.ds(0, count)],
            send_sem=send_sem.at[phase], recv_sem=recv_sem.at[phase],
            device_id={"row": lax.rem(r + 1, nr)}, device_id_type=MESH,
        )

    phases = [
        span(0, a_recv, nr - 1), span(1, ar_recv, nr - 1), span(2, b_recv, nr * nh - 1),
        span(3, br_recv, nh - 1), span(4, st_recv, nr * nh - 1), span(5, d_recv, nr * nh - 1),
        span(6, e_recv, nr - 1),
    ]
    me = r * nh + h

    ld_slot.wait()
    ld_len.wait()
    ld_tok.wait()
    pick_row = iota((batch, batch), 0)
    picked = jnp.zeros((batch, batch), jnp.int32)
    for i in range(batch):
        picked = jnp.where(pick_row == i, slot[i], picked)
    pick = (iota((batch, batch), 1) == picked).astype(F32).astype(BF16)
    chosen = dot_nn(pick, tok[...]).astype(BF16)
    ld_wq.wait()
    part = dot_nn(chosen, wq[...])
    width = NOPE + ROPE
    nope = jnp.concatenate([part[:, width * j : width * j + NOPE] for j in range(hd)], axis=1)
    rope = jnp.concatenate([part[:, width * j + NOPE : width * (j + 1)] for j in range(hd)], axis=1)
    a_send[...] = nope.astype(BF16)
    for k in range(nr):
        ar_send[k] = rope[k * sd : (k + 1) * sd, :]
    pl.semaphore_wait(barrier, len(pairs))
    for dr in order[:-1]:
        send(0, a_send, a_recv.at[dr - 1], dr, 0)
    for dr in order[:-1]:
        send(1, ar_send.at[lax.rem(r + dr, nr)], ar_recv.at[dr - 1], dr, 0)
    n_own = [lens[slot[r * sd + i]] for i in range(sd)]
    half = ROPE // 2
    ld_freq.wait()
    seq_of = lax.rem(iota((rows, half), 0), sd)
    pos = jnp.zeros((rows, half), jnp.int32)
    for i in range(sd):
        pos = jnp.where(seq_of == i, n_own[i] - 1, pos)
    angles = pos.astype(F32) * freq[...]
    cosine = jnp.cos(angles)
    sine = jnp.sin(angles)
    ld_wl.wait()
    phases[0].wait_recv()
    for k in range(nr - 1):
        nope = nope + a_recv[k].astype(F32)

    nope = nope.astype(BF16)
    absorbed = [
        dot_nt(nope[:, NOPE * j : NOPE * (j + 1)], wl[:, (NOPE + V) * j : (NOPE + V) * j + NOPE])
        for j in range(hd)
    ]
    for k in range(nr):
        b_send[k] = jnp.concatenate([x[k * sd : (k + 1) * sd] for x in absorbed], axis=0).astype(BF16)
    for dr, dh in pairs:
        send(2, b_send.at[lax.rem(r + dr, nr)], b_recv.at[me], dr, dh)
    phases[1].wait_recv()
    rope_own = ar_send[r]
    for k in range(nr - 1):
        rope_own = rope_own + ar_recv[k]
    turned = jnp.concatenate([rope_own[:, ROPE * j : ROPE * (j + 1)] for j in range(hd)], axis=0)
    first, second = turned[:, :half], turned[:, half:]
    turned = jnp.concatenate(
        [first * cosine - second * sine, first * sine + second * cosine, jnp.zeros((rows, 128 - ROPE), F32)],
        axis=1,
    ).astype(BF16)
    br_send[...] = turned
    br_recv[h] = turned
    for dh in range(1, nh):
        send(3, br_send, br_recv.at[h], 0, dh)
    b_recv[me] = b_send[r]
    ld_cl.wait()
    ld_cr.wait()
    total_rows = nh * rows
    lane_pos = iota((total_rows, seg), 1) + h * seg
    row_seq = lax.rem(iota((total_rows, seg), 0), sd)
    limit = jnp.zeros((total_rows, seg), jnp.int32)
    for i in range(sd):
        limit = jnp.where(row_seq == i, n_own[i], limit)
    in_range = lane_pos < limit
    phases[2].wait_recv()
    phases[3].wait_recv()

    query = jnp.concatenate(
        [
            jnp.concatenate([b_recv[k * nh + g] for g in range(nh)], axis=0)
            for k in range(nr)
        ],
        axis=1,
    )
    query_rope = jnp.concatenate([br_recv[g] for g in range(nh)], axis=0)[:, :ROPE]
    scores = jnp.zeros((total_rows, seg), F32)
    for i in range(sd):
        s_i = dot_nt(query, cl[i]) + dot_nn(query_rope, cr[i])
        scores = jnp.where(row_seq == i, s_i, scores)
    scores = jnp.where(in_range, scores * np.float32(1.0 / np.sqrt(NOPE + ROPE)), neg_big)
    peak = jnp.max(scores, axis=1, keepdims=True)
    weights = jnp.where(in_range, jnp.exp(scores - peak), 0.0)
    summed = jnp.sum(weights, axis=1, keepdims=True)
    diag = iota((total_rows, 128), 0) == iota((total_rows, 128), 1)
    peak_row = jnp.sum(jnp.where(diag, peak, 0.0), axis=0, keepdims=True)
    sum_row = jnp.sum(jnp.where(diag, summed, 0.0), axis=0, keepdims=True)
    stat = jnp.concatenate([peak_row, sum_row], axis=0)
    st_send[...] = stat
    for dr, dh in pairs:
        send(4, st_send, st_recv.at[me], dr, dh)
    st_recv[me] = stat
    weights = weights.astype(BF16)
    acc = jnp.zeros((total_rows, LAT), F32)
    out_seq = lax.rem(iota((total_rows, LAT), 0), sd)
    for i in range(sd):
        acc = jnp.where(out_seq == i, dot_nn(weights, cl[i]), acc)
    acc = acc.astype(BF16)
    for g in range(nh):
        for k in range(nr):
            d_send[k, g] = acc[g * rows : (g + 1) * rows, k * lb : (k + 1) * lb]
    for dr, dh in pairs:
        send(5, d_send.at[lax.rem(r + dr, nr), lax.rem(h + dh, nh)], d_recv.at[me], dr, dh)
    d_recv[me] = d_send[r, h]
    phases[4].wait_recv()
    own_lane = iota((rows, 128), 1) == iota((rows, 128), 0) + h * rows
    lane_ok = iota((1, 128), 1) < total_rows
    factors = []
    for k in range(nr):
        peaks = [st_recv[k * nh + g, 0:1, :] for g in range(nh)]
        top = functools.reduce(jnp.maximum, peaks)
        scales = [jnp.exp(p - top) for p in peaks]
        total = functools.reduce(
            jnp.add, [st_recv[k * nh + g, 1:2, :] * scales[g] for g in range(nh)]
        )
        inverse = 1.0 / jnp.where(lane_ok, total, 1.0)
        factors.append(
            [
                jnp.sum(jnp.where(own_lane, x * inverse, 0.0), axis=1, keepdims=True)
                for x in scales
            ]
        )
    phases[5].wait_recv()

    latent = [
        functools.reduce(
            jnp.add, [d_recv[k * nh + g].astype(F32) * factors[k][g] for g in range(nh)]
        )
        for k in range(nr)
    ]
    context = jnp.concatenate(
        [
            dot_nn(
                jnp.concatenate([x[sd * j : sd * (j + 1)] for x in latent], axis=0).astype(BF16),
                wl[:, (NOPE + V) * j + NOPE : (NOPE + V) * (j + 1)],
            )
            for j in range(hd)
        ],
        axis=1,
    )
    e_send[...] = context.astype(BF16)
    for dr in order[:-1]:
        send(6, e_send, e_recv.at[dr - 1], dr, 0)
    ld_wo.wait()
    phases[6].wait_recv()
    for k in range(nr - 1):
        context = context + e_recv[k].astype(F32)
    out_part = dot_nt(context.astype(BF16), wo[...])
    for k in range(nr):
        f_send[k] = out_part[k * sd : (k + 1) * sd, :].astype(BF16)

    for k in range(nr):
        mine = jnp.logical_and(r == k, h == r)

        @pl.when(jnp.logical_not(mine))
        def _():
            pltpu.make_async_remote_copy(
                src_ref=f_send.at[k], dst_ref=f_recv.at[h],
                send_sem=send_sem.at[7], recv_sem=recv_sem.at[7],
                device_id={"row": k, "head": r}, device_id_type=MESH,
            ).start()

        @pl.when(mine)
        def _():
            f_recv[h] = f_send[k]

    for c in phases:
        c.wait_send()

    @pl.when(h == r)
    def _():
        span(7, f_recv, nh - 1).wait_recv()

    @pl.when(h != r)
    def _():
        span(7, f_recv, nh).wait_recv()

    out_ref[...] = functools.reduce(jnp.add, [f_recv[g].astype(F32) for g in range(nh)])

    @pl.when(h == r)
    def _():
        span(7, f_send, nr - 1).wait_send()

    @pl.when(h != r)
    def _():
        span(7, f_send, nr).wait_send()


def local_fused(
    nr, nh,
    tokens, query_weight, latent_weight, output_weight, cache_latent, cache_rope, lengths, slot_seq
):
    sd, seg, _ = cache_latent.shape
    hd = query_weight.shape[1] // (NOPE + ROPE)
    batch = nr * sd
    rows = sd * hd
    lb = LAT // nr
    db = query_weight.shape[0]
    half = ROPE // 2
    freq = np.power(10000.0, -2.0 * np.arange(half, dtype=np.float32) / ROPE).astype(np.float32)
    vm = pltpu.VMEM
    dma = pltpu.SemaphoreType.DMA
    scratch = [
        vm((1, half), F32),
        vm((batch, db), BF16),
        vm(query_weight.shape, BF16),
        vm(latent_weight.shape, BF16),
        vm(output_weight.shape, BF16),
        vm(cache_latent.shape, BF16),
        vm(cache_rope.shape, BF16),
        pltpu.SMEM(lengths.shape, jnp.int32),
        pltpu.SMEM(slot_seq.shape, jnp.int32),
        vm((batch, hd * NOPE), BF16),
        vm((nr - 1, batch, hd * NOPE), BF16),
        vm((nr, sd, hd * ROPE), F32),
        vm((nr - 1, sd, hd * ROPE), F32),
        vm((nr, rows, lb), BF16),
        vm((nr * nh, rows, lb), BF16),
        vm((rows, 128), BF16),
        vm((nh, rows, 128), BF16),
        vm((2, 128), F32),
        vm((nr * nh, 2, 128), F32),
        vm((nr, nh, rows, lb), BF16),
        vm((nr * nh, rows, lb), BF16),
        vm((batch, hd * V), BF16),
        vm((nr - 1, batch, hd * V), BF16),
        vm((nr, sd, db), BF16),
        vm((nh, sd, db), BF16),
        dma((9,)),
        dma((8,)),
        dma((8,)),
    ]
    anywhere = pl.BlockSpec(memory_space=pl.ANY)
    summed = pl.pallas_call(
        functools.partial(fused, nr, nh, sd, hd),
        out_shape=pltpu.VMEM((sd, db), F32),
        in_specs=[anywhere] * 9,
        out_specs=pl.BlockSpec(memory_space=pltpu.VMEM),
        scratch_shapes=scratch,
        compiler_params=pltpu.CompilerParams(collective_id=0, has_side_effects=True),
    )(
        jnp.asarray(freq)[None, :], tokens, query_weight, latent_weight, output_weight,
        cache_latent, cache_rope, lengths, slot_seq,
    )
    return summed.astype(BF16)


def solution(mesh):
    placed = (
        P("groups", None),
        P("row", "head"),
        P("row", "head"),
        P("row", "head"),
        P(("groups", "row"), "head", None),
        P(("groups", "row"), None, "head"),
        P("groups"),
        P("groups"),
    )
    nr, nh = mesh.shape["row"], mesh.shape["head"]
    square = nr == nh and nr > 1 and (LAT // nr) % 128 == 0

    def choose(*args):
        query_weight, cache_latent = args[1], args[4]
        rows = cache_latent.shape[0] * (query_weight.shape[1] // (NOPE + ROPE))
        if square and rows % 16 == 0 and rows * nh <= 128:
            return local_fused(nr, nh, *args)
        return local(*args)

    return jax.shard_map(
        choose, mesh=mesh, in_specs=placed, out_specs=P(("groups", "row"), "head"), check_vma=False
    )
```

```python
import functools

import jax
import jax.numpy as jnp
import numpy as np
from jax import lax
from jax.experimental import pallas as pl
from jax.experimental.pallas import tpu as pltpu
from jax.sharding import PartitionSpec as P

D = 2048
H = 16
NOPE = 128
ROPE = 64
V = 128
LAT = 512
BLOCK = 256


neg_big = -1e30


def combined_all(part, axis, combine):
    gathered = jax.tree.map(lambda a: lax.all_gather(a, axis), part)

    def take(source):
        return jax.tree.map(lambda a: lax.dynamic_index_in_dim(a, source, 0, False), gathered)

    return lax.fori_loop(
        1, lax.axis_size(axis), lambda source, state: combine(state, take(source)), take(0)
    )


def absorb(query_weight, output_weight, kv_heads):
    width = query_weight.shape[0]
    head_total = kv_heads.shape[1]
    query_heads = query_weight.reshape(width, head_total, NOPE + ROPE)
    out_heads = output_weight.reshape(width, head_total, V)
    nope_part = jnp.einsum(
        "dhn,lhn->dhl",
        query_heads[:, :, :NOPE],
        kv_heads[:, :, :NOPE],
        preferred_element_type=jnp.float32,
    ).astype(jnp.bfloat16)
    query_abs = jnp.concatenate([nope_part, query_heads[:, :, NOPE:]], axis=2).reshape(width, -1)
    out_abs = jnp.einsum(
        "dhv,lhv->dhl", out_heads, kv_heads[:, :, NOPE:], preferred_element_type=jnp.float32
    ).astype(jnp.bfloat16)
    return (query_abs, out_abs.reshape(width, -1))


def rotate(queries, seq_len):
    half_width = ROPE // 2
    inverse_freq = jnp.power(10000.0, -2.0 * jnp.arange(half_width, dtype=jnp.float32) / ROPE)
    angles = (seq_len - 1).astype(jnp.float32)[:, None] * inverse_freq[None, :]
    cosine = jnp.cos(angles)[:, None, :]
    sine = jnp.sin(angles)[:, None, :]
    first_half = queries[:, :, LAT : LAT + half_width]
    second_half = queries[:, :, LAT + half_width :]
    rotated = jnp.concatenate(
        [first_half * cosine - second_half * sine, first_half * sine + second_half * cosine], axis=2
    )
    return jnp.concatenate([queries[:, :, :LAT], rotated], axis=2)


def combine(earlier, later):
    earlier_max, earlier_sum, earlier_acc = earlier
    later_max, later_sum, later_acc = later
    peak_max = jnp.maximum(earlier_max, later_max)
    earlier_scale = jnp.exp(earlier_max - peak_max)
    later_scale = jnp.exp(later_max - peak_max)
    summed = earlier_sum * earlier_scale + later_sum * later_scale
    weighted = earlier_acc * earlier_scale[..., None] + later_acc * later_scale[..., None]
    return (peak_max, summed, weighted)


def local(
    tokens, query_weight, latent_weight, output_weight, cache_latent, cache_rope, lengths, slot_seq
):
    heads_dev = query_weight.shape[1] // (NOPE + ROPE)
    seq_dev = cache_latent.shape[0]
    seg_len = cache_latent.shape[1]
    latent_full = lax.all_gather(latent_weight, "row", axis=0, tiled=True)
    kv_heads = latent_full.reshape(LAT, heads_dev, NOPE + V)
    full_query, full_out = (
        lax.all_gather(query_weight, "row", axis=0, tiled=True),
        lax.all_gather(output_weight, "row", axis=0, tiled=True),
    )
    query_abs, out_abs = absorb(full_query, full_out, kv_heads)
    first_row = lax.axis_index("row") * seq_dev
    seq_ids = lax.dynamic_slice_in_dim(slot_seq, first_row, seq_dev)
    chosen = tokens[seq_ids]
    seq_len = lengths[seq_ids]
    queries = jnp.dot(chosen, query_abs, preferred_element_type=jnp.float32).reshape(
        seq_dev, heads_dev, LAT + ROPE
    )
    queries = (
        rotate(queries, seq_len).astype(jnp.bfloat16).reshape(seq_dev, heads_dev * (LAT + ROPE))
    )
    queries = lax.all_gather(queries, "head", axis=1, tiled=True).reshape(seq_dev, H, LAT + ROPE)
    query_latent = queries[:, :, :LAT]
    query_rope = queries[:, :, LAT:]
    score_scale = 1.0 / jnp.sqrt(jnp.float32(NOPE + ROPE))
    offset = lax.axis_index("head") * seg_len
    local_len = jnp.clip(seq_len - offset, 0, seg_len)
    live_blocks = (jnp.max(local_len) + BLOCK - 1) // BLOCK

    def advance(block_idx, running):
        run_max, run_sum, run_acc = running
        begin_at = block_idx * BLOCK
        latent_blk = lax.dynamic_slice_in_dim(cache_latent, begin_at, BLOCK, 1)
        rope_blk = lax.dynamic_slice_in_dim(cache_rope, begin_at, BLOCK, 2)
        scores = jnp.einsum(
            "bhl,btl->bht", query_latent, latent_blk, preferred_element_type=jnp.float32
        )
        scores = (
            scores
            + jnp.einsum("bhr,brt->bht", query_rope, rope_blk, preferred_element_type=jnp.float32)
        ) * score_scale
        in_range = (begin_at + jnp.arange(BLOCK, dtype=jnp.int32))[None, None, :] < local_len[
            :, None, None
        ]
        masked = jnp.where(in_range, scores, neg_big)
        new_max = jnp.maximum(run_max, jnp.max(masked, axis=2))
        weights = jnp.where(in_range, jnp.exp(masked - new_max[..., None]), 0.0)
        factor = jnp.exp(run_max - new_max)
        run_sum = run_sum * factor + jnp.sum(weights, axis=2)
        run_acc = run_acc * factor[..., None] + jnp.einsum(
            "bht,btl->bhl",
            weights.astype(jnp.bfloat16),
            latent_blk,
            preferred_element_type=jnp.float32,
        )
        return (new_max, run_sum, run_acc)

    initial = (
        jnp.full((seq_dev, H), neg_big, jnp.float32),
        jnp.zeros((seq_dev, H), jnp.float32),
        jnp.zeros((seq_dev, H, LAT), jnp.float32),
    )
    partial_state = lax.fori_loop(0, live_blocks, advance, initial)
    merged_max, merged_sum, merged_acc = combined_all(partial_state, "head", combine)
    latent_out = (merged_acc / merged_sum[..., None]).astype(jnp.bfloat16)
    own_heads = lax.dynamic_slice_in_dim(
        latent_out, lax.axis_index("head") * heads_dev, heads_dev, 1
    )
    out_term = jnp.einsum(
        "bhl,dhl->bd",
        own_heads,
        out_abs.reshape(D, heads_dev, LAT),
        preferred_element_type=jnp.float32,
    )
    return lax.psum_scatter(out_term, "head", scatter_dimension=1, tiled=True).astype(jnp.bfloat16)


F32 = jnp.float32
BF16 = jnp.bfloat16
MESH = pl.DeviceIdType.MESH


def dot_nn(a, b):
    return lax.dot_general(a, b, (((1,), (0,)), ((), ())), preferred_element_type=F32)


def dot_nt(a, b):
    return lax.dot_general(a, b, (((1,), (1,)), ((), ())), preferred_element_type=F32)


def iota(shape, axis):
    return lax.broadcasted_iota(jnp.int32, shape, axis)


def fused(
    ng, nr, nh, sd, hd,
    freq_h, tok_h, wq_h, wl_h, wo_h, cl_h, cr_h, len_h, slot_h,
    out_ref,
    freq, tok, wq, wl, wo, cl, cr, lens, slot, wv,
    a_send, a_recv, ar_send, ar_recv,
    b_send, b_recv, br_send, br_recv,
    st_send, st_recv, d_send, d_recv,
    e_send, e_recv, f_send, f_recv,
    load_sem,
    send_sem, recv_sem,
):
    r = lax.axis_index("row")
    h = lax.axis_index("head")
    grp = lax.axis_index("groups")
    share = hd // ng
    batch = nr * sd
    rows = sd * hd
    db = wq.shape[0]
    seg = cl.shape[1]
    lb = LAT // nr

    def load(k, src, dst):
        c = pltpu.make_async_copy(src, dst, load_sem.at[k])
        c.start()
        return c

    ld_slot = load(0, slot_h, slot)
    ld_len = load(1, len_h, lens)
    ld_tok = load(2, tok_h.at[:, pl.ds(pl.multiple_of(r * db, 128), db)], tok)
    ld_wq = load(3, wq_h, wq)
    ld_freq = load(4, freq_h, freq)
    ld_wl = load(5, wl_h, wl)
    ld_wv = [
        load(9 + j, wl_h.at[:, pl.ds((NOPE + V) * j + NOPE, V)], wv.at[j, r]) for j in range(hd)
    ]
    ld_cl = load(6, cl_h, cl)
    ld_cr = load(7, cr_h, cr)
    ld_wo = load(8, wo_h, wo)

    order = [dr for dr in range(nr) if dr] + [0]
    pairs = [(dr, dh) for dr in order for dh in range(nh) if dr or dh]
    barrier = pltpu.get_barrier_semaphore()
    for dr, dh in pairs:
        pl.semaphore_signal(
            barrier, inc=1,
            device_id={"row": lax.rem(r + dr, nr), "head": lax.rem(h + dh, nh)},
            device_id_type=MESH,
        )

    for dg in range(1, ng):
        pl.semaphore_signal(
            barrier, inc=1, device_id={"groups": lax.rem(grp + dg, ng)}, device_id_type=MESH
        )

    def send(phase, src, dst, dr, dh):
        pltpu.make_async_remote_copy(
            src_ref=src, dst_ref=dst, send_sem=send_sem.at[phase], recv_sem=recv_sem.at[phase],
            device_id={"row": lax.rem(r + dr, nr), "head": lax.rem(h + dh, nh)},
            device_id_type=MESH,
        ).start()

    def span(phase, ref, count):
        return pltpu.make_async_remote_copy(
            src_ref=ref.at[pl.ds(0, count)], dst_ref=ref.at[pl.ds(0, count)],
            send_sem=send_sem.at[phase], recv_sem=recv_sem.at[phase],
            device_id={"row": lax.rem(r + 1, nr)}, device_id_type=MESH,
        )

    phases = [
        span(0, a_recv, nr - 1), span(1, ar_recv, nr - 1), span(2, b_recv, nr * nh - 1),
        span(3, br_recv, nh - 1), span(4, st_recv, nh - 1), span(5, d_recv, nh - 1),
        span(6, e_recv, nr - 1),
    ]
    me = r * nh + h

    def spread(p):
        j = grp * share + p
        for dr in order[:-1]:
            send(8 + p, wv.at[j, r], wv.at[j, r], dr, 0)

    def swap(p):
        j = grp * share + p
        span(8 + p, wv.at[0], nr - 1).wait_recv()
        for dg in range(1, ng):
            for dr in order[:-1]:
                k = lax.rem(r + dr, nr)
                pltpu.make_async_remote_copy(
                    src_ref=wv.at[j, k], dst_ref=wv.at[j, k],
                    send_sem=send_sem.at[8 + share + p], recv_sem=recv_sem.at[8 + share + p],
                    device_id={"groups": lax.rem(grp + dg, ng)}, device_id_type=MESH,
                ).start()

    for p in range(share):
        phases.append(span(8 + p, wv.at[0], nr - 1))
        phases.append(span(8 + share + p, wv.at[0], nr - 1))

    ld_slot.wait()
    ld_len.wait()
    ld_tok.wait()
    pick_row = iota((batch, batch), 0)
    picked = jnp.zeros((batch, batch), jnp.int32)
    for i in range(batch):
        picked = jnp.where(pick_row == i, slot[i], picked)
    pick = (iota((batch, batch), 1) == picked).astype(F32).astype(BF16)
    chosen = dot_nn(pick, tok[...]).astype(BF16)
    ld_wq.wait()
    part = dot_nn(chosen, wq[...])
    width = NOPE + ROPE
    nope = jnp.concatenate([part[:, width * j : width * j + NOPE] for j in range(hd)], axis=1)
    rope = jnp.concatenate([part[:, width * j + NOPE : width * (j + 1)] for j in range(hd)], axis=1)
    a_send[...] = nope.astype(BF16)
    for k in range(nr):
        ar_send[k] = rope[k * sd : (k + 1) * sd, :]
    for x in ld_wv:
        x.wait()
    pl.semaphore_wait(barrier, len(pairs) + ng - 1)
    for dr in order[:-1]:
        send(0, a_send, a_recv.at[dr - 1], dr, 0)
    for dr in order[:-1]:
        send(1, ar_send.at[lax.rem(r + dr, nr)], ar_recv.at[dr - 1], dr, 0)
    spread(0)
    n_own = [lens[slot[r * sd + i]] for i in range(sd)]
    half = ROPE // 2
    ld_freq.wait()
    seq_of = lax.rem(iota((rows, half), 0), sd)
    pos = jnp.zeros((rows, half), jnp.int32)
    for i in range(sd):
        pos = jnp.where(seq_of == i, n_own[i] - 1, pos)
    angles = pos.astype(F32) * freq[...]
    cosine = jnp.cos(angles)
    sine = jnp.sin(angles)
    ld_wl.wait()
    phases[0].wait_recv()
    for k in range(nr - 1):
        nope = nope + a_recv[k].astype(F32)

    nope = nope.astype(BF16)
    absorbed = [
        dot_nt(nope[:, NOPE * j : NOPE * (j + 1)], wl[:, (NOPE + V) * j : (NOPE + V) * j + NOPE])
        for j in range(hd)
    ]
    for k in range(nr):
        b_send[k] = jnp.concatenate([x[k * sd : (k + 1) * sd] for x in absorbed], axis=0).astype(BF16)
    for dr, dh in pairs:
        send(2, b_send.at[lax.rem(r + dr, nr)], b_recv.at[me], dr, dh)
    phases[1].wait_recv()
    rope_own = ar_send[r]
    for k in range(nr - 1):
        rope_own = rope_own + ar_recv[k]
    turned = jnp.concatenate([rope_own[:, ROPE * j : ROPE * (j + 1)] for j in range(hd)], axis=0)
    first, second = turned[:, :half], turned[:, half:]
    turned = jnp.concatenate(
        [first * cosine - second * sine, first * sine + second * cosine, jnp.zeros((rows, 128 - ROPE), F32)],
        axis=1,
    ).astype(BF16)
    br_send[...] = turned
    br_recv[h] = turned
    for dh in range(1, nh):
        send(3, br_send, br_recv.at[h], 0, dh)
    for p in range(1, share):
        spread(p)
    swap(0)
    b_recv[me] = b_send[r]
    ld_cl.wait()
    ld_cr.wait()
    total_rows = nh * rows
    lane_pos = iota((total_rows, seg), 1) + h * seg
    row_seq = lax.rem(iota((total_rows, seg), 0), sd)
    limit = jnp.zeros((total_rows, seg), jnp.int32)
    for i in range(sd):
        limit = jnp.where(row_seq == i, n_own[i], limit)
    in_range = lane_pos < limit
    phases[2].wait_recv()
    phases[3].wait_recv()

    query = jnp.concatenate(
        [
            jnp.concatenate([b_recv[k * nh + g] for g in range(nh)], axis=0)
            for k in range(nr)
        ],
        axis=1,
    )
    query_rope = jnp.concatenate([br_recv[g] for g in range(nh)], axis=0)[:, :ROPE]
    scores = jnp.zeros((total_rows, seg), F32)
    for i in range(sd):
        s_i = dot_nt(query, cl[i]) + dot_nn(query_rope, cr[i])
        scores = jnp.where(row_seq == i, s_i, scores)
    scores = jnp.where(in_range, scores * np.float32(1.0 / np.sqrt(NOPE + ROPE)), neg_big)
    peak = jnp.max(scores, axis=1, keepdims=True)
    weights = jnp.where(in_range, jnp.exp(scores - peak), 0.0)
    summed = jnp.sum(weights, axis=1, keepdims=True)
    diag = iota((total_rows, 128), 0) == iota((total_rows, 128), 1)
    peak_row = jnp.sum(jnp.where(diag, peak, 0.0), axis=0, keepdims=True)
    sum_row = jnp.sum(jnp.where(diag, summed, 0.0), axis=0, keepdims=True)
    stat = jnp.concatenate([peak_row, sum_row], axis=0)
    st_send[...] = stat
    for dh in range(1, nh):
        send(4, st_send, st_recv.at[h], 0, dh)
    st_recv[h] = stat
    weights = weights.astype(BF16)
    acc = jnp.zeros((total_rows, LAT), F32)
    out_seq = lax.rem(iota((total_rows, LAT), 0), sd)
    for i in range(sd):
        acc = jnp.where(out_seq == i, dot_nn(weights, cl[i]), acc)
    acc = acc.astype(BF16)
    for g in range(nh):
        d_send[g] = acc[g * rows : (g + 1) * rows]
    for dh in range(1, nh):
        send(5, d_send.at[lax.rem(h + dh, nh)], d_recv.at[h], 0, dh)
    d_recv[h] = d_send[h]
    for p in range(1, share):
        swap(p)
    phases[4].wait_recv()
    own_lane = iota((rows, 128), 1) == iota((rows, 128), 0) + h * rows
    lane_ok = iota((1, 128), 1) < total_rows
    peaks = [st_recv[g, 0:1, :] for g in range(nh)]
    top = functools.reduce(jnp.maximum, peaks)
    scales = [jnp.exp(p - top) for p in peaks]
    total = functools.reduce(jnp.add, [st_recv[g, 1:2, :] * scales[g] for g in range(nh)])
    inverse = 1.0 / jnp.where(lane_ok, total, 1.0)
    factors = [
        jnp.sum(jnp.where(own_lane, x * inverse, 0.0), axis=1, keepdims=True) for x in scales
    ]
    phases[5].wait_recv()

    latent = functools.reduce(
        jnp.add, [d_recv[g].astype(F32) * factors[g] for g in range(nh)]
    )
    for p in range(share):
        span(8 + share + p, wv.at[0], nr - 1).wait_recv()
    context = jnp.concatenate(
        [
            dot_nn(latent[sd * j : sd * (j + 1)].astype(BF16), wv[j].reshape(nr * lb, V))
            for j in range(hd)
        ],
        axis=1,
    ).astype(BF16)
    e_send[...] = context
    for dr in order[:-1]:
        send(6, e_send, e_recv.at[r], dr, 0)
    e_recv[r] = context
    ld_wo.wait()
    phases[6].wait_recv()
    context = jnp.concatenate([e_recv[k].astype(F32) for k in range(nr)], axis=0)
    out_part = dot_nt(context.astype(BF16), wo[...])
    for k in range(nr):
        f_send[k] = out_part[k * sd : (k + 1) * sd, :].astype(BF16)

    for k in range(nr):
        mine = jnp.logical_and(r == k, h == r)

        @pl.when(jnp.logical_not(mine))
        def _():
            pltpu.make_async_remote_copy(
                src_ref=f_send.at[k], dst_ref=f_recv.at[h],
                send_sem=send_sem.at[7], recv_sem=recv_sem.at[7],
                device_id={"row": k, "head": r}, device_id_type=MESH,
            ).start()

        @pl.when(mine)
        def _():
            f_recv[h] = f_send[k]

    for c in phases:
        c.wait_send()

    @pl.when(h == r)
    def _():
        span(7, f_recv, nh - 1).wait_recv()

    @pl.when(h != r)
    def _():
        span(7, f_recv, nh).wait_recv()

    out_ref[...] = functools.reduce(jnp.add, [f_recv[g].astype(F32) for g in range(nh)])

    @pl.when(h == r)
    def _():
        span(7, f_send, nr - 1).wait_send()

    @pl.when(h != r)
    def _():
        span(7, f_send, nr).wait_send()


def local_fused(
    ng, nr, nh,
    tokens, query_weight, latent_weight, output_weight, cache_latent, cache_rope, lengths, slot_seq
):
    sd, seg, _ = cache_latent.shape
    hd = query_weight.shape[1] // (NOPE + ROPE)
    batch = nr * sd
    rows = sd * hd
    lb = LAT // nr
    db = query_weight.shape[0]
    half = ROPE // 2
    freq = np.power(10000.0, -2.0 * np.arange(half, dtype=np.float32) / ROPE).astype(np.float32)
    share = hd // ng
    vm = pltpu.VMEM
    dma = pltpu.SemaphoreType.DMA
    scratch = [
        vm((1, half), F32),
        vm((batch, db), BF16),
        vm(query_weight.shape, BF16),
        vm(latent_weight.shape, BF16),
        vm(output_weight.shape, BF16),
        vm(cache_latent.shape, BF16),
        vm(cache_rope.shape, BF16),
        pltpu.SMEM(lengths.shape, jnp.int32),
        pltpu.SMEM(slot_seq.shape, jnp.int32),
        vm((hd, nr, lb, V), BF16),
        vm((batch, hd * NOPE), BF16),
        vm((nr - 1, batch, hd * NOPE), BF16),
        vm((nr, sd, hd * ROPE), F32),
        vm((nr - 1, sd, hd * ROPE), F32),
        vm((nr, rows, lb), BF16),
        vm((nr * nh, rows, lb), BF16),
        vm((rows, 128), BF16),
        vm((nh, rows, 128), BF16),
        vm((2, 128), F32),
        vm((nh, 2, 128), F32),
        vm((nh, rows, LAT), BF16),
        vm((nh, rows, LAT), BF16),
        vm((sd, hd * V), BF16),
        vm((nr, sd, hd * V), BF16),
        vm((nr, sd, db), BF16),
        vm((nh, sd, db), BF16),
        dma((9 + hd,)),
        dma((8 + 2 * share,)),
        dma((8 + 2 * share,)),
    ]
    anywhere = pl.BlockSpec(memory_space=pl.ANY)
    summed = pl.pallas_call(
        functools.partial(fused, ng, nr, nh, sd, hd),
        out_shape=pltpu.VMEM((sd, db), F32),
        in_specs=[anywhere] * 9,
        out_specs=pl.BlockSpec(memory_space=pltpu.VMEM),
        scratch_shapes=scratch,
        compiler_params=pltpu.CompilerParams(collective_id=0, has_side_effects=True),
    )(
        jnp.asarray(freq)[None, :], tokens, query_weight, latent_weight, output_weight,
        cache_latent, cache_rope, lengths, slot_seq,
    )
    return summed.astype(BF16)


def solution(mesh):
    placed = (
        P("groups", None),
        P("row", "head"),
        P("row", "head"),
        P("row", "head"),
        P(("groups", "row"), "head", None),
        P(("groups", "row"), None, "head"),
        P("groups"),
        P("groups"),
    )
    ng, nr, nh = (mesh.shape[a] for a in ("groups", "row", "head"))
    square = ng == 2 and nr == nh and nr > 1 and (LAT // nr) % 128 == 0

    def choose(*args):
        query_weight, cache_latent = args[1], args[4]
        hd = query_weight.shape[1] // (NOPE + ROPE)
        rows = cache_latent.shape[0] * hd
        if square and hd % ng == 0 and rows % 16 == 0 and rows * nh <= 128:
            return local_fused(ng, nr, nh, *args)
        return local(*args)

    return jax.shard_map(
        choose, mesh=mesh, in_specs=placed, out_specs=P(("groups", "row"), "head"), check_vma=False
    )
```

```python
import functools

import jax
import jax.numpy as jnp
import numpy as np
from jax import lax
from jax.experimental import pallas as pl
from jax.experimental.pallas import tpu as pltpu
from jax.sharding import PartitionSpec as P

D = 2048
H = 16
NOPE = 128
ROPE = 64
V = 128
LAT = 512
BLOCK = 256


neg_big = -1e30


def combined_all(part, axis, combine):
    gathered = jax.tree.map(lambda a: lax.all_gather(a, axis), part)

    def take(source):
        return jax.tree.map(lambda a: lax.dynamic_index_in_dim(a, source, 0, False), gathered)

    return lax.fori_loop(
        1, lax.axis_size(axis), lambda source, state: combine(state, take(source)), take(0)
    )


def absorb(query_weight, output_weight, kv_heads):
    width = query_weight.shape[0]
    head_total = kv_heads.shape[1]
    query_heads = query_weight.reshape(width, head_total, NOPE + ROPE)
    out_heads = output_weight.reshape(width, head_total, V)
    nope_part = jnp.einsum(
        "dhn,lhn->dhl",
        query_heads[:, :, :NOPE],
        kv_heads[:, :, :NOPE],
        preferred_element_type=jnp.float32,
    ).astype(jnp.bfloat16)
    query_abs = jnp.concatenate([nope_part, query_heads[:, :, NOPE:]], axis=2).reshape(width, -1)
    out_abs = jnp.einsum(
        "dhv,lhv->dhl", out_heads, kv_heads[:, :, NOPE:], preferred_element_type=jnp.float32
    ).astype(jnp.bfloat16)
    return (query_abs, out_abs.reshape(width, -1))


def rotate(queries, seq_len):
    half_width = ROPE // 2
    inverse_freq = jnp.power(10000.0, -2.0 * jnp.arange(half_width, dtype=jnp.float32) / ROPE)
    angles = (seq_len - 1).astype(jnp.float32)[:, None] * inverse_freq[None, :]
    cosine = jnp.cos(angles)[:, None, :]
    sine = jnp.sin(angles)[:, None, :]
    first_half = queries[:, :, LAT : LAT + half_width]
    second_half = queries[:, :, LAT + half_width :]
    rotated = jnp.concatenate(
        [first_half * cosine - second_half * sine, first_half * sine + second_half * cosine], axis=2
    )
    return jnp.concatenate([queries[:, :, :LAT], rotated], axis=2)


def combine(earlier, later):
    earlier_max, earlier_sum, earlier_acc = earlier
    later_max, later_sum, later_acc = later
    peak_max = jnp.maximum(earlier_max, later_max)
    earlier_scale = jnp.exp(earlier_max - peak_max)
    later_scale = jnp.exp(later_max - peak_max)
    summed = earlier_sum * earlier_scale + later_sum * later_scale
    weighted = earlier_acc * earlier_scale[..., None] + later_acc * later_scale[..., None]
    return (peak_max, summed, weighted)


def local(
    tokens, query_weight, latent_weight, output_weight, cache_latent, cache_rope, lengths, slot_seq
):
    heads_dev = query_weight.shape[1] // (NOPE + ROPE)
    seq_dev = cache_latent.shape[0]
    seg_len = cache_latent.shape[1]
    latent_full = lax.all_gather(latent_weight, "row", axis=0, tiled=True)
    kv_heads = latent_full.reshape(LAT, heads_dev, NOPE + V)
    full_query, full_out = (
        lax.all_gather(query_weight, "row", axis=0, tiled=True),
        lax.all_gather(output_weight, "row", axis=0, tiled=True),
    )
    query_abs, out_abs = absorb(full_query, full_out, kv_heads)
    first_row = lax.axis_index("row") * seq_dev
    seq_ids = lax.dynamic_slice_in_dim(slot_seq, first_row, seq_dev)
    chosen = tokens[seq_ids]
    seq_len = lengths[seq_ids]
    queries = jnp.dot(chosen, query_abs, preferred_element_type=jnp.float32).reshape(
        seq_dev, heads_dev, LAT + ROPE
    )
    queries = (
        rotate(queries, seq_len).astype(jnp.bfloat16).reshape(seq_dev, heads_dev * (LAT + ROPE))
    )
    queries = lax.all_gather(queries, "head", axis=1, tiled=True).reshape(seq_dev, H, LAT + ROPE)
    query_latent = queries[:, :, :LAT]
    query_rope = queries[:, :, LAT:]
    score_scale = 1.0 / jnp.sqrt(jnp.float32(NOPE + ROPE))
    offset = lax.axis_index("head") * seg_len
    local_len = jnp.clip(seq_len - offset, 0, seg_len)
    live_blocks = (jnp.max(local_len) + BLOCK - 1) // BLOCK

    def advance(block_idx, running):
        run_max, run_sum, run_acc = running
        begin_at = block_idx * BLOCK
        latent_blk = lax.dynamic_slice_in_dim(cache_latent, begin_at, BLOCK, 1)
        rope_blk = lax.dynamic_slice_in_dim(cache_rope, begin_at, BLOCK, 2)
        scores = jnp.einsum(
            "bhl,btl->bht", query_latent, latent_blk, preferred_element_type=jnp.float32
        )
        scores = (
            scores
            + jnp.einsum("bhr,brt->bht", query_rope, rope_blk, preferred_element_type=jnp.float32)
        ) * score_scale
        in_range = (begin_at + jnp.arange(BLOCK, dtype=jnp.int32))[None, None, :] < local_len[
            :, None, None
        ]
        masked = jnp.where(in_range, scores, neg_big)
        new_max = jnp.maximum(run_max, jnp.max(masked, axis=2))
        weights = jnp.where(in_range, jnp.exp(masked - new_max[..., None]), 0.0)
        factor = jnp.exp(run_max - new_max)
        run_sum = run_sum * factor + jnp.sum(weights, axis=2)
        run_acc = run_acc * factor[..., None] + jnp.einsum(
            "bht,btl->bhl",
            weights.astype(jnp.bfloat16),
            latent_blk,
            preferred_element_type=jnp.float32,
        )
        return (new_max, run_sum, run_acc)

    initial = (
        jnp.full((seq_dev, H), neg_big, jnp.float32),
        jnp.zeros((seq_dev, H), jnp.float32),
        jnp.zeros((seq_dev, H, LAT), jnp.float32),
    )
    partial_state = lax.fori_loop(0, live_blocks, advance, initial)
    merged_max, merged_sum, merged_acc = combined_all(partial_state, "head", combine)
    latent_out = (merged_acc / merged_sum[..., None]).astype(jnp.bfloat16)
    own_heads = lax.dynamic_slice_in_dim(
        latent_out, lax.axis_index("head") * heads_dev, heads_dev, 1
    )
    out_term = jnp.einsum(
        "bhl,dhl->bd",
        own_heads,
        out_abs.reshape(D, heads_dev, LAT),
        preferred_element_type=jnp.float32,
    )
    return lax.psum_scatter(out_term, "head", scatter_dimension=1, tiled=True).astype(jnp.bfloat16)


F32 = jnp.float32
BF16 = jnp.bfloat16
MESH = pl.DeviceIdType.MESH


def dot_nn(a, b):
    return lax.dot_general(a, b, (((1,), (0,)), ((), ())), preferred_element_type=F32)


def dot_nt(a, b):
    return lax.dot_general(a, b, (((1,), (1,)), ((), ())), preferred_element_type=F32)


def iota(shape, axis):
    return lax.broadcasted_iota(jnp.int32, shape, axis)


def fused(
    nr, nh, sd, hd,
    freq_h, tok_h, wq_h, wl_h, wo_h, cl_h, cr_h, len_h, slot_h,
    out_ref,
    freq, tok, wq, wl, wo, cl, cr, lens, slot,
    a_send, a_recv, ar_send, ar_recv,
    b_send, b_recv, br_send, br_recv,
    st_send, st_recv, d_send, d_recv,
    e_send, e_recv, f_send, f_recv,
    load_sem,
    send_sem, recv_sem,
):
    r = lax.axis_index("row")
    h = lax.axis_index("head")
    batch = nr * sd
    rows = sd * hd
    db = wq.shape[0]
    seg = cl.shape[1]
    lb = LAT // nr

    def load(k, src, dst):
        c = pltpu.make_async_copy(src, dst, load_sem.at[k])
        c.start()
        return c

    ld_slot = load(0, slot_h, slot)
    ld_len = load(1, len_h, lens)
    ld_tok = load(2, tok_h.at[:, pl.ds(pl.multiple_of(r * db, 128), db)], tok)
    ld_wq = load(3, wq_h, wq)
    ld_freq = load(4, freq_h, freq)
    ld_wl = load(5, wl_h, wl)
    ld_cl = load(6, cl_h, cl)
    ld_cr = load(7, cr_h, cr)
    ld_wo = load(8, wo_h, wo)

    order = []
    high = lax.div(2 * r, nr)
    for k in range(nr - 1):
        down = nr - 1 - k
        down = down - 1 + lax.div(down - r + nr - 1, nr)
        up = k + lax.div(k - r + nr, nr)
        order.append(lax.rem((1 - high) * down + high * up - r + nr, nr))
    order.append(0)
    pairs = [(dr, dh) for dr in order for dh in range(nh) if dr is not order[-1] or dh]
    barrier = pltpu.get_barrier_semaphore()
    for dr, dh in pairs:
        pl.semaphore_signal(
            barrier, inc=1,
            device_id={"row": lax.rem(r + dr, nr), "head": lax.rem(h + dh, nh)},
            device_id_type=MESH,
        )

    def send(phase, src, dst, dr, dh):
        pltpu.make_async_remote_copy(
            src_ref=src, dst_ref=dst, send_sem=send_sem.at[phase], recv_sem=recv_sem.at[phase],
            device_id={"row": lax.rem(r + dr, nr), "head": lax.rem(h + dh, nh)},
            device_id_type=MESH,
        ).start()

    def span(phase, ref, count):
        return pltpu.make_async_remote_copy(
            src_ref=ref.at[pl.ds(0, count)], dst_ref=ref.at[pl.ds(0, count)],
            send_sem=send_sem.at[phase], recv_sem=recv_sem.at[phase],
            device_id={"row": lax.rem(r + 1, nr)}, device_id_type=MESH,
        )

    phases = [
        span(0, a_recv, nr - 1), span(1, ar_recv, nr - 1), span(2, b_recv, nr * nh - 1),
        span(3, br_recv, nh - 1), span(4, st_recv, nr * nh - 1), span(5, d_recv, nr * nh - 1),
        span(6, e_recv, nr - 1),
    ]
    me = r * nh + h

    ld_slot.wait()
    ld_len.wait()
    ld_tok.wait()
    pick_row = iota((batch, batch), 0)
    picked = jnp.zeros((batch, batch), jnp.int32)
    for i in range(batch):
        picked = jnp.where(pick_row == i, slot[i], picked)
    pick = (iota((batch, batch), 1) == picked).astype(F32).astype(BF16)
    chosen = dot_nn(pick, tok[...]).astype(BF16)
    ld_wq.wait()
    part = dot_nn(chosen, wq[...])
    width = NOPE + ROPE
    nope = jnp.concatenate([part[:, width * j : width * j + NOPE] for j in range(hd)], axis=1)
    rope = jnp.concatenate([part[:, width * j + NOPE : width * (j + 1)] for j in range(hd)], axis=1)
    a_send[...] = nope.astype(BF16)
    for k in range(nr):
        ar_send[k] = rope[k * sd : (k + 1) * sd, :]
    pl.semaphore_wait(barrier, len(pairs))
    for dr in order[:-1]:
        send(0, a_send, a_recv.at[dr - 1], dr, 0)
    for dr in order[:-1]:
        send(1, ar_send.at[lax.rem(r + dr, nr)], ar_recv.at[dr - 1], dr, 0)
    n_own = [lens[slot[r * sd + i]] for i in range(sd)]
    half = ROPE // 2
    ld_freq.wait()
    seq_of = lax.rem(iota((rows, half), 0), sd)
    pos = jnp.zeros((rows, half), jnp.int32)
    for i in range(sd):
        pos = jnp.where(seq_of == i, n_own[i] - 1, pos)
    angles = pos.astype(F32) * freq[...]
    cosine = jnp.cos(angles)
    sine = jnp.sin(angles)
    ld_wl.wait()
    phases[0].wait_recv()
    for k in range(nr - 1):
        nope = nope + a_recv[k].astype(F32)

    nope = nope.astype(BF16)
    absorbed = [
        dot_nt(nope[:, NOPE * j : NOPE * (j + 1)], wl[:, (NOPE + V) * j : (NOPE + V) * j + NOPE])
        for j in range(hd)
    ]
    for k in range(nr):
        b_send[k] = jnp.concatenate([x[k * sd : (k + 1) * sd] for x in absorbed], axis=0).astype(BF16)
    for dr, dh in pairs:
        send(2, b_send.at[lax.rem(r + dr, nr)], b_recv.at[me], dr, dh)
    phases[1].wait_recv()
    rope_own = ar_send[r]
    for k in range(nr - 1):
        rope_own = rope_own + ar_recv[k]
    turned = jnp.concatenate([rope_own[:, ROPE * j : ROPE * (j + 1)] for j in range(hd)], axis=0)
    first, second = turned[:, :half], turned[:, half:]
    turned = jnp.concatenate(
        [first * cosine - second * sine, first * sine + second * cosine, jnp.zeros((rows, 128 - ROPE), F32)],
        axis=1,
    ).astype(BF16)
    br_send[...] = turned
    br_recv[h] = turned
    for dh in range(1, nh):
        send(3, br_send, br_recv.at[h], 0, dh)
    b_recv[me] = b_send[r]
    ld_cl.wait()
    ld_cr.wait()
    total_rows = nh * rows
    lane_pos = iota((total_rows, seg), 1) + h * seg
    row_seq = lax.rem(iota((total_rows, seg), 0), sd)
    limit = jnp.zeros((total_rows, seg), jnp.int32)
    for i in range(sd):
        limit = jnp.where(row_seq == i, n_own[i], limit)
    in_range = lane_pos < limit
    phases[2].wait_recv()
    phases[3].wait_recv()

    query = jnp.concatenate(
        [
            jnp.concatenate([b_recv[k * nh + g] for g in range(nh)], axis=0)
            for k in range(nr)
        ],
        axis=1,
    )
    query_rope = jnp.concatenate([br_recv[g] for g in range(nh)], axis=0)[:, :ROPE]
    scores = jnp.zeros((total_rows, seg), F32)
    for i in range(sd):
        s_i = dot_nt(query, cl[i]) + dot_nn(query_rope, cr[i])
        scores = jnp.where(row_seq == i, s_i, scores)
    scores = jnp.where(in_range, scores * np.float32(1.0 / np.sqrt(NOPE + ROPE)), neg_big)
    peak = jnp.max(scores, axis=1, keepdims=True)
    weights = jnp.where(in_range, jnp.exp(scores - peak), 0.0)
    summed = jnp.sum(weights, axis=1, keepdims=True)
    diag = iota((total_rows, 128), 0) == iota((total_rows, 128), 1)
    peak_row = jnp.sum(jnp.where(diag, peak, 0.0), axis=0, keepdims=True)
    sum_row = jnp.sum(jnp.where(diag, summed, 0.0), axis=0, keepdims=True)
    stat = jnp.concatenate([peak_row, sum_row], axis=0)
    st_send[...] = stat
    for dr, dh in pairs:
        send(4, st_send, st_recv.at[me], dr, dh)
    st_recv[me] = stat
    spread = jnp.concatenate(
        [jnp.where(row_seq == i, weights, 0.0).astype(BF16) for i in range(sd)], axis=1
    )
    acc = dot_nn(spread, cl[...].reshape(sd * seg, LAT)).astype(BF16)
    for g in range(nh):
        for k in range(nr):
            d_send[k, g] = acc[g * rows : (g + 1) * rows, k * lb : (k + 1) * lb]
    for dr, dh in pairs:
        send(5, d_send.at[lax.rem(r + dr, nr), lax.rem(h + dh, nh)], d_recv.at[me], dr, dh)
    d_recv[me] = d_send[r, h]
    phases[4].wait_recv()
    own_lane = iota((rows, 128), 1) == iota((rows, 128), 0) + h * rows
    lane_ok = iota((1, 128), 1) < total_rows
    factors = []
    for k in range(nr):
        peaks = [st_recv[k * nh + g, 0:1, :] for g in range(nh)]
        top = functools.reduce(jnp.maximum, peaks)
        scales = [jnp.exp(p - top) for p in peaks]
        total = functools.reduce(
            jnp.add, [st_recv[k * nh + g, 1:2, :] * scales[g] for g in range(nh)]
        )
        inverse = 1.0 / jnp.where(lane_ok, total, 1.0)
        factors.append(
            [
                jnp.sum(jnp.where(own_lane, x * inverse, 0.0), axis=1, keepdims=True)
                for x in scales
            ]
        )
    phases[5].wait_recv()

    latent = [
        functools.reduce(
            jnp.add, [d_recv[k * nh + g].astype(F32) * factors[k][g] for g in range(nh)]
        )
        for k in range(nr)
    ]
    context = jnp.concatenate(
        [
            dot_nn(
                jnp.concatenate([x[sd * j : sd * (j + 1)] for x in latent], axis=0).astype(BF16),
                wl[:, (NOPE + V) * j + NOPE : (NOPE + V) * (j + 1)],
            )
            for j in range(hd)
        ],
        axis=1,
    )
    e_send[...] = context.astype(BF16)
    for dr in order[:-1]:
        send(6, e_send, e_recv.at[dr - 1], dr, 0)
    ld_wo.wait()
    phases[6].wait_recv()
    for k in range(nr - 1):
        context = context + e_recv[k].astype(F32)
    out_part = dot_nt(context.astype(BF16), wo[...])
    for k in range(nr):
        f_send[k] = out_part[k * sd : (k + 1) * sd, :].astype(BF16)

    for k in range(nr):
        mine = jnp.logical_and(r == k, h == r)

        @pl.when(jnp.logical_not(mine))
        def _():
            pltpu.make_async_remote_copy(
                src_ref=f_send.at[k], dst_ref=f_recv.at[h],
                send_sem=send_sem.at[7], recv_sem=recv_sem.at[7],
                device_id={"row": k, "head": r}, device_id_type=MESH,
            ).start()

        @pl.when(mine)
        def _():
            f_recv[h] = f_send[k]

    for c in phases:
        c.wait_send()

    @pl.when(h == r)
    def _():
        span(7, f_recv, nh - 1).wait_recv()

    @pl.when(h != r)
    def _():
        span(7, f_recv, nh).wait_recv()

    out_ref[...] = functools.reduce(jnp.add, [f_recv[g].astype(F32) for g in range(nh)])

    @pl.when(h == r)
    def _():
        span(7, f_send, nr - 1).wait_send()

    @pl.when(h != r)
    def _():
        span(7, f_send, nr).wait_send()


def local_fused(
    nr, nh,
    tokens, query_weight, latent_weight, output_weight, cache_latent, cache_rope, lengths, slot_seq
):
    sd, seg, _ = cache_latent.shape
    hd = query_weight.shape[1] // (NOPE + ROPE)
    batch = nr * sd
    rows = sd * hd
    lb = LAT // nr
    db = query_weight.shape[0]
    half = ROPE // 2
    freq = np.power(10000.0, -2.0 * np.arange(half, dtype=np.float32) / ROPE).astype(np.float32)
    vm = pltpu.VMEM
    dma = pltpu.SemaphoreType.DMA
    scratch = [
        vm((1, half), F32),
        vm((batch, db), BF16),
        vm(query_weight.shape, BF16),
        vm(latent_weight.shape, BF16),
        vm(output_weight.shape, BF16),
        vm(cache_latent.shape, BF16),
        vm(cache_rope.shape, BF16),
        pltpu.SMEM(lengths.shape, jnp.int32),
        pltpu.SMEM(slot_seq.shape, jnp.int32),
        vm((batch, hd * NOPE), BF16),
        vm((nr - 1, batch, hd * NOPE), BF16),
        vm((nr, sd, hd * ROPE), F32),
        vm((nr - 1, sd, hd * ROPE), F32),
        vm((nr, rows, lb), BF16),
        vm((nr * nh, rows, lb), BF16),
        vm((rows, 128), BF16),
        vm((nh, rows, 128), BF16),
        vm((2, 128), F32),
        vm((nr * nh, 2, 128), F32),
        vm((nr, nh, rows, lb), BF16),
        vm((nr * nh, rows, lb), BF16),
        vm((batch, hd * V), BF16),
        vm((nr - 1, batch, hd * V), BF16),
        vm((nr, sd, db), BF16),
        vm((nh, sd, db), BF16),
        dma((9,)),
        dma((8,)),
        dma((8,)),
    ]
    anywhere = pl.BlockSpec(memory_space=pl.ANY)
    summed = pl.pallas_call(
        functools.partial(fused, nr, nh, sd, hd),
        out_shape=pltpu.VMEM((sd, db), F32),
        in_specs=[anywhere] * 9,
        out_specs=pl.BlockSpec(memory_space=pltpu.VMEM),
        scratch_shapes=scratch,
        compiler_params=pltpu.CompilerParams(collective_id=0, has_side_effects=True),
    )(
        jnp.asarray(freq)[None, :], tokens, query_weight, latent_weight, output_weight,
        cache_latent, cache_rope, lengths, slot_seq,
    )
    return summed.astype(BF16)


def solution(mesh):
    placed = (
        P("groups", None),
        P("row", "head"),
        P("row", "head"),
        P("row", "head"),
        P(("groups", "row"), "head", None),
        P(("groups", "row"), None, "head"),
        P("groups"),
        P("groups"),
    )
    nr, nh = mesh.shape["row"], mesh.shape["head"]
    square = nr == nh and nr > 1 and (LAT // nr) % 128 == 0

    def choose(*args):
        query_weight, cache_latent = args[1], args[4]
        rows = cache_latent.shape[0] * (query_weight.shape[1] // (NOPE + ROPE))
        if square and rows % 16 == 0 and rows * nh <= 128:
            return local_fused(nr, nh, *args)
        return local(*args)

    return jax.shard_map(
        choose, mesh=mesh, in_specs=placed, out_specs=P(("groups", "row"), "head"), check_vma=False
    )
```
